256 devices in a mesh: vrow: 32 (over z, y), vcol: 8 (over x, core).
Axes of the slice: x: 4, y: 4, z: 8, core: 2. Of those that a mesh axis runs over, the one named last changes fastest.
Arguments:
- policy_hidden: bfloat16 [1024, 3584], P(None, 'vcol'), may hold values from -400 to 400
- ref_hidden: bfloat16 [1024, 3584], P(None, 'vcol'), may hold values from -400 to 400
- mix_num: int32 [1024], replicated, may hold values from 0 to 16, as said below
- mix_den: int32 [1024], replicated, may hold values from 2 to 16
- policy_unembed: bfloat16 [3584, 131072], P(None, ('vrow', 'vcol')), may hold values from -0.09375 to 0.09375
- ref_unembed: bfloat16 [3584, 131072], P(None, ('vrow', 'vcol')), may hold values from -0.09375 to 0.09375
Outputs:
- mix_logprobs: float32 [1024, 131072], P(None, ('vrow', 'vcol'))
The draws below stay inside these ranges and needn't reach their ends.
Inputs may be any that keep to these rules, and one draw needn't show every extreme that they name: Each sequence's mix_num is at most its mix_den.
All inputs are finite; a program needn't handle non-finite values.
Results may differ from the reference program's by a relative error of at most 0.0003.
Values may be sent and summed in bfloat16 or wider, within the bound.
A program may use at most 64 MiB of HBM per device.

```python
import jax
import jax.numpy as jnp

D = 3584
B = 1024
VOCAB = 131072


def weight_pair(key):
    base = jax.random.fold_in(key, 7)
    first, second = jax.random.split(base)
    denom = jax.random.randint(first, (B,), 2, 17)
    numer = jax.random.randint(second, (B,), 0, 17) % (denom + 1)
    return (numer.astype(jnp.int32), denom.astype(jnp.int32))


def draw_mix_num(key, part):
    return weight_pair(key)[0]


def draw_mix_den(key, part):
    return weight_pair(key)[1]


def hidden_law(key, salt):
    base = jax.random.fold_in(key, salt)
    first = jax.random.fold_in(base, 0)
    values = 3.0 * jax.random.normal(first, (B, D), jnp.float32)
    return jnp.clip(values, -400.0, 400.0).astype(jnp.bfloat16)


def draw_policy_hidden(key, part):
    return hidden_law(key, 11)


def draw_ref_hidden(key, part):
    return hidden_law(key, 13)


def block_scale(own_key, shape, cuts, least, largest):
    def one(dim, shards_of):
        heights = jax.random.uniform(jax.random.fold_in(jax.random.fold_in(own_key, 6), dim), (shards_of,), jnp.float32, least / len(cuts), largest / len(cuts))
        return jnp.repeat(jnp.exp(heights), shape[dim] // shards_of).reshape((-1,) + (1,) * (len(shape) - dim - 1))

    level = one(*cuts[0])
    for cut in cuts[1:]:
        level = level * one(*cut)
    return level


def gaussian(rng, dims, deviation, bound, shards=(), held_as=jnp.bfloat16):
    level = block_scale(rng, dims, shards, -0.22, 0.18) if shards else 1.0
    result = jax.random.normal(rng, dims, jnp.float32) * deviation * level
    return jnp.minimum(jnp.maximum(result, -bound), bound).astype(held_as)


def setup_inputs(seed: int = 0) -> dict:
    key_of = jax.random.split(jax.random.key(seed), 7)
    return {
        "policy_hidden": draw_policy_hidden(jax.random.fold_in(key_of[6], 71), 0),
        "ref_hidden": draw_ref_hidden(jax.random.fold_in(key_of[6], 71), 0),
        "mix_num": draw_mix_num(jax.random.fold_in(key_of[6], 71), 0),
        "mix_den": draw_mix_den(jax.random.fold_in(key_of[6], 71), 0),
        "policy_unembed": gaussian(key_of[4], (D, VOCAB), D ** -0.5, 0.09375, ((1, 256),)),
        "ref_unembed": gaussian(key_of[5], (D, VOCAB), D ** -0.5, 0.09375, ((1, 256),)),
    }


def reference(policy_hidden, ref_hidden, mix_num, mix_den, policy_unembed, ref_unembed):
    policy_logits = jnp.dot(policy_hidden, policy_unembed, preferred_element_type=jnp.float32)
    ref_logits = jnp.dot(ref_hidden, ref_unembed, preferred_element_type=jnp.float32)
    beta = (mix_num.astype(jnp.float32) / mix_den.astype(jnp.float32))[:, None]
    mixed = (1.0 - beta) * policy_logits + beta * ref_logits
    top = jnp.max(mixed, axis=1, keepdims=True)
    total = jnp.sum(jnp.exp(mixed - top), axis=1, keepdims=True)
    return mixed - top - jnp.log(total)
```

```python
import functools

import jax
import jax.numpy as jnp
from jax import lax
from jax.experimental import pallas as pl
from jax.experimental.pallas import tpu as pltpu
from jax.sharding import Mesh
from jax.sharding import PartitionSpec as P

MESH = pl.DeviceIdType.MESH
VCOL = ("vcol_0", "vcol_1")
VROW_VCOL = ("vrow_0", "vrow_1", "vcol_0", "vcol_1")

HALF = 512
QUARTER = 128
CHUNK = 32
PIECES = QUARTER // CHUNK
FEATS = 448
FULL = 384
WIRE = 2 * FEATS
LAG = 3

XP, XM, YP, YM, ZP, ZM = range(6)


def place(flow, r):
    if flow in (XP, YP, YM):
        early, mid = 2, 6
    else:
        early, mid = 4, 7
    if r < 2 * PIECES:
        slot, piece = early + r % 2, r // 2
    elif r < 3 * PIECES:
        slot, piece = mid, r - 2 * PIECES
    else:
        slot, piece = {XP: 2, XM: 5, YP: 3, YM: 6, ZP: 4, ZM: 7}[flow], r - 3 * PIECES
    if r >= 3 * PIECES:
        return slot, 2, piece
    return slot, {XP: 0, XM: 0, YP: 1, YM: 3, ZP: 1, ZM: 3}[flow], piece


def kernel(
    ph, rh, num, den, pw, rw, mixed, lse,
    buf, other, raw, wb, acc, beta, stat, xyin, stat2, zin, part, partin,
    hid_sem, w_sem, wr_sem, ws_sem, recv_sem, send_sem, peer_sem, out_sem, xy_sem, z_sem, l_sem,
):
    z, y = lax.axis_index("vrow_0"), lax.axis_index("vrow_1")
    x, c = lax.axis_index("vcol_0"), lax.axis_index("vcol_1")
    o = 1 - c
    colour = (y + z) % 4
    xs = [x, (x + 1) % 4, (x + 3) % 4, (x + 2) % 4]
    target = {
        XP: (z, y, (x + 3) % 4, c),
        XM: (z, y, (x + 1) % 4, c),
        YP: (z, (y + 3) % 4, x, c),
        YM: (z, (y + 1) % 4, x, c),
        ZP: ((z + 7) % 8, y, x, c),
        ZM: ((z + 1) % 8, y, x, c),
    }
    peer = (z, y, x, o)

    def remote(src, dst, send, recv, device):
        return pltpu.make_async_remote_copy(
            src_ref=src, dst_ref=dst, send_sem=send, recv_sem=recv, device_id=device, device_id_type=MESH
        )

    mine = pl.ds(pl.multiple_of(c * HALF, HALF), HALF)
    theirs = pl.ds(pl.multiple_of(o * HALF, HALF), HALF)
    hidden = [
        pltpu.make_async_copy(ph, raw.at[0], hid_sem.at[0]),
        pltpu.make_async_copy(rh, raw.at[1], hid_sem.at[1]),
        pltpu.make_async_copy(ph.at[mine, pl.ds(0, FULL)], buf.at[0, :, pl.ds(0, FULL)], hid_sem.at[2]),
        pltpu.make_async_copy(rh.at[mine, pl.ds(0, FULL)], buf.at[0, :, pl.ds(512, FULL)], hid_sem.at[3]),
        pltpu.make_async_copy(ph.at[theirs, pl.ds(0, FULL)], other.at[:, pl.ds(0, FULL)], hid_sem.at[4]),
        pltpu.make_async_copy(rh.at[theirs, pl.ds(0, FULL)], other.at[:, pl.ds(512, FULL)], hid_sem.at[5]),
    ]
    for copy in hidden:
        copy.start()

    barrier = pltpu.get_barrier_semaphore()
    near = [target[f] for f in range(6)]
    near += [(z, y, (x + 3) % 4, o), (z, y, (x + 1) % 4, o), peer]
    for device in near:
        pl.semaphore_signal(barrier, inc=1, device_id=device, device_id_type=MESH)

    def weight_parts(base, dst):
        base = pl.multiple_of(base * FEATS, 64)
        return [
            (pw.at[pl.ds(base, FEATS)], dst.at[pl.ds(0, FEATS)]),
            (rw.at[pl.ds(base + FULL, 64)], dst.at[pl.ds(576, 64)]),
            (rw.at[pl.ds(base, FULL)], dst.at[pl.ds(640, FULL)]),
        ]

    for slot in range(8):
        base = xs[slot // 2] * 2 + (c if slot % 2 == 0 else o)
        for src, dst in weight_parts(base, wb.at[0, slot]):
            pltpu.make_async_copy(src, dst, w_sem.at[slot]).start()

    for k in range(4):
        row = pl.ds(c * 4 + k, 1)
        value = num[row, :].astype(jnp.float32) / den[row, :].astype(jnp.float32)
        beta[pl.ds(k * QUARTER, QUARTER), :] = jnp.broadcast_to(value, (QUARTER, 128)).T
    for h in range(2):
        for slot in range(8):
            wb[h, slot, pl.ds(FEATS, 128), :] = jnp.zeros((128, HALF), jnp.bfloat16)

    for copy in hidden:
        copy.wait()
    buf[0, :, pl.ds(FULL, 128)] = jnp.concatenate(
        [raw[0, mine, pl.ds(FULL, 64)], raw[1, mine, pl.ds(FULL, 64)]], axis=1
    )
    other[:, pl.ds(FULL, 128)] = jnp.concatenate(
        [raw[0, theirs, pl.ds(FULL, 64)], raw[1, theirs, pl.ds(FULL, 64)]], axis=1
    )
    pl.semaphore_wait(barrier, len(near))

    def rows(offset, piece):
        quarter = (colour + offset) % 4
        return pl.ds(pl.multiple_of(quarter * QUARTER + piece * CHUNK, CHUNK), CHUNK)

    def send(flow, r, src, cross=False):
        slot, _, _ = place(flow, r)
        source, window = src
        device = target[flow]
        if cross:
            device = (*device[:3], o)
        remote(source.at[window], buf.at[slot, window], send_sem.at[flow], recv_sem.at[flow, r], device).start()

    def arrived(flow, r):
        slot, offset, piece = place(flow, r)
        ref = buf.at[slot, rows(offset, piece)]
        remote(ref, ref, send_sem.at[flow], recv_sem.at[flow, r], target[flow]).wait_recv()
        return buf.at[slot], rows(offset, piece)

    for k in range(PIECES):
        for flow in (XP, XM):
            send(flow, 2 * k, (buf.at[0], rows(0, k)))
            send(flow, 2 * k + 1, (other, rows(0, k)), cross=True)
    swap = remote(other, buf.at[1], peer_sem.at[0], peer_sem.at[1], peer)
    swap.start()
    for slot in range(8):
        base = xs[slot // 2] * 2 + (o if slot % 2 == 0 else c)
        for src, dst in weight_parts(base, wb.at[1, slot]):
            remote(src, dst, ws_sem, wr_sem.at[slot], peer).start()

    seen = set()

    def weights(slot):
        if slot in seen:
            return
        seen.add(slot)
        own, got = wb.at[0, slot, pl.ds(0, WIRE)], wb.at[1, slot, pl.ds(0, WIRE)]
        pltpu.make_async_copy(own, own, w_sem.at[slot]).wait()
        remote(got, got, ws_sem, wr_sem.at[slot], peer).wait_recv()

    def block(offset):
        quarter = (colour + offset) % 4
        return pl.ds(pl.multiple_of(quarter * QUARTER, QUARTER), QUARTER)

    def multiply(slot, offsets, first=False):
        weights(slot)
        parts = [buf[slot, block(i), :] for i in offsets]
        left = parts[0] if len(parts) == 1 else jnp.concatenate(parts, axis=0)
        for h in range(2):
            policy = jnp.dot(left[:, :512], wb[h, slot, pl.ds(0, 512), :], preferred_element_type=jnp.float32)
            ref = jnp.dot(left[:, 384:], wb[h, slot, pl.ds(512, 512), :], preferred_element_type=jnp.float32)
            for n, i in enumerate(offsets):
                b = jnp.concatenate([beta[block(i), :]] * 4, axis=1)
                at = slice(n * QUARTER, (n + 1) * QUARTER)
                value = (1.0 - b) * policy[at] + b * ref[at]
                acc[h, block(i), :] = value if first else acc[h, block(i), :] + value

    def out_rows(offset):
        quarter = (colour + offset) % 4
        return pl.ds(pl.multiple_of(c * HALF + quarter * QUARTER, QUARTER), QUARTER)

    def out_copies(offset):
        near = pltpu.make_async_copy(acc.at[0, block(offset)], mixed.at[out_rows(offset)], out_sem.at[0, offset])
        far = remote(
            acc.at[1, block(offset)], mixed.at[out_rows(offset)], out_sem.at[1, offset], out_sem.at[2, offset], peer
        )
        return near, far

    def finish(offset):
        tiles = [acc[h, block(offset), pl.ds(j * 128, 128)] for h in range(2) for j in range(4)]
        high = functools.reduce(jnp.maximum, tiles)
        total = functools.reduce(jnp.add, [jnp.exp(t - high) for t in tiles])
        high, total = high.T, total.T
        top = jnp.max(high, axis=0, keepdims=True)
        summed = jnp.sum(total * jnp.exp(high - top), axis=0, keepdims=True)
        quarter = (colour + offset) % 4
        stat[pl.ds(quarter, 1), :] = top
        stat[pl.ds(quarter + 4, 1), :] = summed
        for copy in out_copies(offset):
            copy.start()

    def spread(r):
        plus, minus = arrived(XP, r), arrived(XM, r)
        if r < 3 * PIECES:
            for flow in (YP, YM):
                send(flow, r, plus)
            for flow in (ZP, ZM):
                send(flow, r, minus)
        if r < 2 * PIECES:
            if r % 2 == 0:
                send(XP, 2 * PIECES + r // 2, plus)
            else:
                send(XM, 2 * PIECES + r // 2, minus)
        if 2 * PIECES <= r < 3 * PIECES:
            k = r - 2 * PIECES
            send(XP, 3 * PIECES + k, (buf.at[0], rows(2, k)))
            send(XM, 3 * PIECES + k, (other, rows(2, k)), cross=True)

    def relay(r):
        got = {flow: arrived(flow, r) for flow in (YP, YM, ZP, ZM)}
        if r < 2 * PIECES:
            if r % 2 == 1:
                send(YP, 3 * PIECES + r // 2, got[YP])
            else:
                send(ZP, 3 * PIECES + r // 2, got[ZP])
        elif r < 3 * PIECES:
            send(YM, PIECES + r, got[YM])
            send(ZM, PIECES + r, got[ZM])

    tasks = {
        0: [lambda: multiply(0, (0, 1, 2, 3), first=True)],
        3: [lambda: (swap.wait_recv(), multiply(1, (0, 1, 2, 3)))],
        7: [lambda: multiply(2, (0,)), lambda: multiply(3, (0,))],
        8: [lambda: multiply(4, (0,)), lambda: multiply(5, (0,))],
        10: [lambda: multiply(2, (1, 3))],
        11: [lambda: multiply(3, (1, 3)), lambda: multiply(4, (1, 3))],
        12: [lambda: multiply(5, (1, 3)), lambda: multiply(6, (0,))],
        13: [lambda: multiply(7, (0,))],
        14: [lambda: multiply(6, (1, 3)), lambda: finish(0)],
        15: [lambda: multiply(7, (1, 3)), lambda: multiply(2, (2,))],
        16: [lambda: multiply(5, (2,)), lambda: finish(1)],
        17: [lambda: finish(3)],
        18: [lambda: multiply(s, (2,)) for s in (3, 4, 6, 7)] + [lambda: finish(2)],
    }
    tasks[18] = [functools.partial(multiply, s, (2,)) for s in (3, 4, 6, 7)] + [lambda: finish(2)]
    for r in range(4 * PIECES + LAG):
        if r < 4 * PIECES:
            spread(r)
        if r >= LAG:
            relay(r - LAG)
        for task in tasks.get(r, ()):
            task()

    def combine(pairs):
        top = functools.reduce(jnp.maximum, [p[0] for p in pairs])
        return top, functools.reduce(jnp.add, [p[1] * jnp.exp(p[0] - top) for p in pairs])

    def halves(ref):
        return ref[pl.ds(0, 4), :], ref[pl.ds(4, 4), :]

    sends = []
    for k in range(1, 16):
        device = (z, (y + k // 4) % 4, (x + k % 4) % 4, c)
        sends.append(remote(stat, xyin.at[k], xy_sem.at[0, k], xy_sem.at[1, k], device))
        sends[-1].start()
    for copy in sends:
        copy.wait_recv()
    top, total = combine([halves(stat)] + [halves(xyin.at[k]) for k in range(1, 16)])
    stat2[pl.ds(0, 4), :] = top
    stat2[pl.ds(4, 4), :] = total
    for k in range(1, 8):
        copy = remote(stat2, zin.at[k], z_sem.at[0, k], z_sem.at[1, k], ((z + k) % 8, y, x, c))
        copy.start()
        sends.append(copy)
    for copy in sends[15:]:
        copy.wait_recv()
    top, total = combine([(top, total)] + [halves(zin.at[k]) for k in range(1, 8)])
    value = top + jnp.log(total)
    part[pl.ds(0, 4), :] = value
    part[pl.ds(4, 4), :] = value
    last = remote(part, partin, l_sem.at[0], l_sem.at[1], peer)
    last.start()
    lse[c] = part[...]

    for copy in sends:
        copy.wait_send()
    for flow in range(6):
        remote(buf.at[0], buf.at[0], send_sem.at[flow], recv_sem.at[flow, 0], peer).wait_send()
    gone = wb.at[0, :, pl.ds(0, WIRE)]
    remote(gone, gone, ws_sem, wr_sem.at[0], peer).wait_send()
    swap.wait_send()
    for offset in range(4):
        near, far = out_copies(offset)
        near.wait()
        far.wait()
    last.wait()
    lse[o] = partin[...]


def body(policy_hidden, ref_hidden, mix_num, mix_den, policy_unembed, ref_unembed):
    hbm = pl.BlockSpec(memory_space=pl.ANY)
    vmem = pl.BlockSpec(memory_space=pltpu.VMEM)
    dma = pltpu.SemaphoreType.DMA
    mixed, lse = pl.pallas_call(
        kernel,
        out_shape=(
            jax.ShapeDtypeStruct((2 * HALF, HALF), jnp.float32),
            jax.ShapeDtypeStruct((2, 8, 128), jnp.float32),
        ),
        in_specs=[hbm, hbm, vmem, vmem, hbm, hbm],
        out_specs=(hbm, vmem),
        scratch_shapes=[
            pltpu.VMEM((8, HALF, WIRE), jnp.bfloat16),
            pltpu.VMEM((HALF, WIRE), jnp.bfloat16),
            pltpu.VMEM((2, 2 * HALF, FEATS), jnp.bfloat16),
            pltpu.VMEM((2, 8, 1024, HALF), jnp.bfloat16),
            pltpu.VMEM((2, HALF, HALF), jnp.float32),
            pltpu.VMEM((HALF, 128), jnp.float32),
            pltpu.VMEM((8, 128), jnp.float32),
            pltpu.VMEM((16, 8, 128), jnp.float32),
            pltpu.VMEM((8, 128), jnp.float32),
            pltpu.VMEM((8, 8, 128), jnp.float32),
            pltpu.VMEM((8, 128), jnp.float32),
            pltpu.VMEM((8, 128), jnp.float32),
            dma((6,)),
            dma((8,)),
            dma((8,)),
            dma(()),
            dma((6, 4 * PIECES)),
            dma((6,)),
            dma((2,)),
            dma((3, 4)),
            dma((2, 16)),
            dma((2, 8)),
            dma((2,)),
        ],
        compiler_params=pltpu.CompilerParams(collective_id=0, has_side_effects=True),
        name="mixture",
    )(
        policy_hidden,
        ref_hidden,
        mix_num.reshape(8, 128),
        mix_den.reshape(8, 128),
        policy_unembed,
        ref_unembed,
    )
    return mixed - lse[:, :4].reshape(2 * HALF, 1)


def solution(mesh):
    finer = Mesh(mesh.devices.reshape(8, 4, 4, 2), VROW_VCOL)
    placed = (P(None, VCOL), P(None, VCOL), P(), P(), P(None, VROW_VCOL), P(None, VROW_VCOL))
    return jax.shard_map(
        body, mesh=finer, in_specs=placed, out_specs=P(None, VROW_VCOL), check_vma=False
    )
```

```python
import functools

import jax
import jax.numpy as jnp
from jax import lax
from jax.experimental import pallas as pl
from jax.experimental.pallas import tpu as pltpu
from jax.sharding import Mesh
from jax.sharding import PartitionSpec as P

MESH = pl.DeviceIdType.MESH
VCOL = ("vcol_0", "vcol_1")
VROW_VCOL = ("vrow_0", "vrow_1", "vcol_0", "vcol_1")

HALF = 512
QUARTER = 128
CHUNK = 32
PIECES = QUARTER // CHUNK
FEATS = 448
FULL = 384
WIRE = 2 * FEATS
GROUP = (0, 1, 2, 2, 3, 3, 4, 4)
LAG = 3

XP, XM, YP, YM, ZP, ZM = range(6)


def place(flow, r):
    if flow in (XP, YP, YM):
        early, mid = 2, 6
    else:
        early, mid = 4, 7
    if r < 2 * PIECES:
        slot, piece = early + r % 2, r // 2
    elif r < 3 * PIECES:
        slot, piece = mid, r - 2 * PIECES
    else:
        slot, piece = {XP: 2, XM: 5, YP: 3, YM: 6, ZP: 4, ZM: 7}[flow], r - 3 * PIECES
    if r >= 3 * PIECES:
        return slot, 2, piece
    return slot, {XP: 0, XM: 0, YP: 1, YM: 3, ZP: 1, ZM: 3}[flow], piece


def kernel(
    ph, rh, num, den, pw, rw, out,
    buf, other, raw, wb, acc, theirs, ratio, beta, stat, xyin, stat2, zin,
    hid_sem, w_sem, wr_sem, ws_sem, recv_sem, send_sem, peer_sem, far_sem, xy_sem, z_sem,
):
    z, y = lax.axis_index("vrow_0"), lax.axis_index("vrow_1")
    x, c = lax.axis_index("vcol_0"), lax.axis_index("vcol_1")
    o = 1 - c
    colour = (y + z) % 4
    xs = [x, (x + 1) % 4, (x + 3) % 4, (x + 2) % 4]
    target = {
        XP: (z, y, (x + 3) % 4, c),
        XM: (z, y, (x + 1) % 4, c),
        YP: (z, (y + 3) % 4, x, c),
        YM: (z, (y + 1) % 4, x, c),
        ZP: ((z + 7) % 8, y, x, c),
        ZM: ((z + 1) % 8, y, x, c),
    }
    peer = (z, y, x, o)

    def remote(src, dst, send, recv, device):
        return pltpu.make_async_remote_copy(
            src_ref=src, dst_ref=dst, send_sem=send, recv_sem=recv, device_id=device, device_id_type=MESH
        )

    def lanes(core, offset):
        return pl.ds(pl.multiple_of((core * 4 + (colour + offset) % 4) * QUARTER, QUARTER), QUARTER)

    for i in range(4):
        for n, core in enumerate((c, o)):
            at = lanes(core, i)
            pltpu.make_async_copy(ph.at[:, at], raw.at[0, :, at], hid_sem.at[min(i, 1)]).start()
            pltpu.make_async_copy(rh.at[:, at], raw.at[1, :, at], hid_sem.at[min(i, 1)]).start()

    pltpu.make_async_copy(num, ratio.at[0], hid_sem.at[2]).start()
    pltpu.make_async_copy(den, ratio.at[1], hid_sem.at[2]).start()

    barrier = pltpu.get_barrier_semaphore()
    near = [target[f] for f in range(6)]
    near += [(z, y, (x + 3) % 4, o), (z, y, (x + 1) % 4, o), peer]
    for device in near:
        pl.semaphore_signal(barrier, inc=1, device_id=device, device_id_type=MESH)

    def weight_parts(base, dst):
        base = pl.multiple_of(base * FEATS, 64)
        return [
            (pw.at[pl.ds(base, FEATS)], dst.at[pl.ds(0, FEATS)]),
            (rw.at[pl.ds(base + FULL, 64)], dst.at[pl.ds(576, 64)]),
            (rw.at[pl.ds(base, FULL)], dst.at[pl.ds(640, FULL)]),
        ]

    def block(offset):
        quarter = (colour + offset) % 4
        return pl.ds(pl.multiple_of(quarter * QUARTER, QUARTER), QUARTER)

    def loaded(k, blocks):
        here = raw.at[:, :, pl.ds(0, blocks * QUARTER)]
        pltpu.make_async_copy(here, here, hid_sem.at[k]).wait()

    def pack(i):
        for n, core in enumerate((c, o)):
            at = lanes(core, i)
            turned = jnp.concatenate(
                [raw[0, :, at], raw[1, pl.ds(FULL, 64), at], raw[1, pl.ds(0, FULL), at]], axis=0
            ).T
            if n == 0:
                buf[0, block(i), :] = turned
            else:
                other[block(i), :] = turned

    loaded(0, 2)
    pack(0)
    pl.semaphore_wait(barrier, len(near))

    def rows(offset, piece):
        quarter = (colour + offset) % 4
        return pl.ds(pl.multiple_of(quarter * QUARTER + piece * CHUNK, CHUNK), CHUNK)

    def send(flow, r, src, cross=False):
        slot, _, _ = place(flow, r)
        source, window = src
        device = target[flow]
        if cross:
            device = (*device[:3], o)
        remote(source.at[window], buf.at[slot, window], send_sem.at[flow], recv_sem.at[flow, r], device).start()

    def arrived(flow, r):
        slot, offset, piece = place(flow, r)
        ref = buf.at[slot, rows(offset, piece)]
        remote(ref, ref, send_sem.at[flow], recv_sem.at[flow, r], target[flow]).wait_recv()
        return buf.at[slot], rows(offset, piece)

    for k in range(PIECES):
        for flow in (XP, XM):
            send(flow, 2 * k, (buf.at[0], rows(0, k)))
            send(flow, 2 * k + 1, (other, rows(0, k)), cross=True)
    def fetch(slots):
        for slot in slots:
            base = xs[slot // 2] * 2 + (o if slot % 2 == 0 else c)
            for src, dst in weight_parts(base, wb.at[1, slot]):
                remote(src, dst, ws_sem, wr_sem.at[GROUP[slot]], peer).start()
        for slot in slots:
            base = xs[slot // 2] * 2 + (c if slot % 2 == 0 else o)
            for src, dst in weight_parts(base, wb.at[0, slot]):
                pltpu.make_async_copy(src, dst, w_sem).start()

    fetch((0,))
    loaded(1, 6)
    for i in range(1, 4):
        pack(i)
    swap = remote(other, buf.at[1], peer_sem.at[0], peer_sem.at[1], peer)
    swap.start()
    fetch(range(1, 8))

    pltpu.make_async_copy(ratio, ratio, hid_sem.at[2]).wait()
    for k in range(4):
        row = pl.ds(c * 4 + k, 1)
        value = ratio[0, row, :].astype(jnp.float32) / ratio[1, row, :].astype(jnp.float32)
        beta[pl.ds(k * QUARTER, QUARTER), :] = jnp.broadcast_to(value, (QUARTER, 128)).T
    for h in range(2):
        for slot in range(8):
            wb[h, slot, pl.ds(FEATS, 128), :] = jnp.zeros((128, HALF), jnp.bfloat16)

    seen = set()

    def weights(slot):
        if not seen:
            own = wb.at[0, :, pl.ds(0, WIRE)]
            pltpu.make_async_copy(own, own, w_sem).wait()
        group = GROUP[slot]
        if group in seen:
            return
        seen.add(group)
        got = wb.at[1, pl.ds(GROUP.index(group), GROUP.count(group)), pl.ds(0, WIRE)]
        remote(got, got, ws_sem, wr_sem.at[group], peer).wait_recv()

    def multiply(slot, offsets, first=False):
        weights(slot)
        parts = [buf[slot, block(i), :] for i in offsets]
        left = parts[0] if len(parts) == 1 else jnp.concatenate(parts, axis=0)
        for h in range(2):
            policy = jnp.dot(left[:, :512], wb[h, slot, pl.ds(0, 512), :], preferred_element_type=jnp.float32)
            ref = jnp.dot(left[:, 384:], wb[h, slot, pl.ds(512, 512), :], preferred_element_type=jnp.float32)
            for n, i in enumerate(offsets):
                b = jnp.concatenate([beta[block(i), :]] * 4, axis=1)
                at = slice(n * QUARTER, (n + 1) * QUARTER)
                value = (1.0 - b) * policy[at] + b * ref[at]
                acc[h, block(i), :] = value if first else acc[h, block(i), :] + value

    def swap_rows(offset):
        return remote(
            acc.at[1, block(offset)], theirs.at[block(offset)], far_sem.at[0], far_sem.at[1], peer
        )

    def finish(offset):
        tiles = [acc[h, block(offset), pl.ds(j * 128, 128)] for h in range(2) for j in range(4)]
        high = functools.reduce(jnp.maximum, tiles)
        total = functools.reduce(jnp.add, [jnp.exp(t - high) for t in tiles])
        high, total = high.T, total.T
        top = jnp.max(high, axis=0, keepdims=True)
        summed = jnp.sum(total * jnp.exp(high - top), axis=0, keepdims=True)
        quarter = (colour + offset) % 4
        stat[pl.ds(quarter, 1), :] = top
        stat[pl.ds(quarter + 4, 1), :] = summed
        swap_rows(offset).start()

    def spread(r):
        if r >= 3 * PIECES:
            k = r - 3 * PIECES
            for flow in (YP, ZP):
                slot, _, _ = place(flow, r)
                send(flow, r, (buf.at[slot], rows(1, k)))
        plus, minus = arrived(XP, r), arrived(XM, r)
        if r < 3 * PIECES:
            for flow in (YP, YM):
                send(flow, r, plus)
            for flow in (ZP, ZM):
                send(flow, r, minus)
        if r < 2 * PIECES:
            if r % 2 == 0:
                send(XP, 2 * PIECES + r // 2, plus)
            else:
                send(XM, 2 * PIECES + r // 2, minus)
        if 2 * PIECES <= r < 3 * PIECES:
            k = r - 2 * PIECES
            send(XP, 3 * PIECES + k, (buf.at[0], rows(2, k)))
            send(XM, 3 * PIECES + k, (other, rows(2, k)), cross=True)

    def relay(r):
        got = {flow: arrived(flow, r) for flow in (YP, YM, ZP, ZM)}
        if 2 * PIECES <= r < 3 * PIECES:
            send(YM, PIECES + r, got[YM])
            send(ZM, PIECES + r, got[ZM])

    tasks = {
        0: [lambda: multiply(0, (0, 1, 2, 3), first=True)],
        3: [lambda: (swap.wait_recv(), multiply(1, (0, 1, 2, 3)))],
        7: [lambda: multiply(2, (0,)), lambda: multiply(3, (0,))],
        8: [lambda: multiply(4, (0,)), lambda: multiply(5, (0,))],
        10: [lambda: multiply(2, (1, 3))],
        11: [lambda: multiply(3, (1, 3)), lambda: multiply(4, (1, 3))],
        12: [lambda: multiply(5, (1, 3)), lambda: multiply(6, (0,))],
        13: [lambda: multiply(7, (0,))],
        14: [lambda: multiply(6, (1, 3)), lambda: finish(0)],
        15: [lambda: multiply(7, (1, 3)), lambda: multiply(2, (2,))],
        16: [lambda: multiply(5, (2,)), lambda: finish(1)],
        17: [lambda: finish(3)],
    }
    tasks[18] = [functools.partial(multiply, s, (2,)) for s in (3, 4, 6, 7)] + [lambda: finish(2)]
    for r in range(4 * PIECES + LAG):
        if r < 4 * PIECES:
            spread(r)
        if r >= LAG:
            relay(r - LAG)
        for task in tasks.get(r, ()):
            task()

    def combine(pairs):
        top = functools.reduce(jnp.maximum, [p[0] for p in pairs])
        return top, functools.reduce(jnp.add, [p[1] * jnp.exp(p[0] - top) for p in pairs])

    def halves(ref):
        return ref[pl.ds(0, 4), :], ref[pl.ds(4, 4), :]

    for k in range(1, 16):
        device = (z, (y + k // 4) % 4, (x + k % 4) % 4, c)
        remote(stat, xyin.at[k], xy_sem.at[0], xy_sem.at[1], device).start()
    plane = xyin.at[pl.ds(1, 15)]
    plane = remote(plane, plane, xy_sem.at[0], xy_sem.at[1], peer)
    plane.wait_recv()
    top, total = combine([halves(stat)] + [halves(xyin.at[k]) for k in range(1, 16)])
    stat2[pl.ds(0, 4), :] = top
    stat2[pl.ds(4, 4), :] = total
    for k in range(1, 16):
        device = ((z + k % 8) % 8, y, x, c if k < 8 else o)
        remote(stat2, zin.at[k], z_sem.at[0], z_sem.at[1], device).start()
    line = zin.at[pl.ds(1, 15)]
    line = remote(line, line, z_sem.at[0], z_sem.at[1], peer)
    line.wait_recv()
    top, total = combine([(top, total)] + [halves(zin.at[k]) for k in range(1, 8)])
    value = top + jnp.log(total)
    top, total = combine([halves(zin.at[k]) for k in range(8, 16)])
    other_value = top + jnp.log(total)
    swapped = remote(theirs, theirs, far_sem.at[0], far_sem.at[1], peer)
    swapped.wait_recv()
    for i in range(4):
        at = pl.ds(i * QUARTER, QUARTER)
        for core, source, log in ((c, acc.at[0], value), (o, theirs, other_value)):
            column = jnp.broadcast_to(log[i : i + 1, :], (QUARTER, 128)).T
            here = pl.ds(pl.multiple_of(core * HALF + i * QUARTER, QUARTER), QUARTER)
            out[here, :] = source[at, :] - jnp.concatenate([column] * 4, axis=1)

    plane.wait_send()
    line.wait_send()
    for flow in range(6):
        remote(buf.at[0], buf.at[0], send_sem.at[flow], recv_sem.at[flow, 0], peer).wait_send()
    gone = wb.at[0, :, pl.ds(0, WIRE)]
    remote(gone, gone, ws_sem, wr_sem.at[0], peer).wait_send()
    swap.wait_send()
    swapped.wait_send()


def body(policy_hidden, ref_hidden, mix_num, mix_den, policy_unembed, ref_unembed):
    hbm = pl.BlockSpec(memory_space=pltpu.HBM)
    vmem = pl.BlockSpec(memory_space=pltpu.VMEM)
    stay = functools.partial(pltpu.with_memory_space_constraint, memory_space=pltpu.HBM)
    dma = pltpu.SemaphoreType.DMA
    return pl.pallas_call(
        kernel,
        out_shape=pltpu.VMEM((2 * HALF, HALF), jnp.float32),
        in_specs=[hbm] * 6,
        out_specs=vmem,
        scratch_shapes=[
            pltpu.VMEM((8, HALF, WIRE), jnp.bfloat16),
            pltpu.VMEM((HALF, WIRE), jnp.bfloat16),
            pltpu.VMEM((2, FEATS, 2 * HALF), jnp.bfloat16),
            pltpu.VMEM((2, 8, 1024, HALF), jnp.bfloat16),
            pltpu.VMEM((2, HALF, HALF), jnp.float32),
            pltpu.VMEM((HALF, HALF), jnp.float32),
            pltpu.VMEM((2, 8, 128), jnp.int32),
            pltpu.VMEM((HALF, 128), jnp.float32),
            pltpu.VMEM((8, 128), jnp.float32),
            pltpu.VMEM((16, 8, 128), jnp.float32),
            pltpu.VMEM((8, 128), jnp.float32),
            pltpu.VMEM((16, 8, 128), jnp.float32),
            dma((3,)),
            dma(()),
            dma((5,)),
            dma(()),
            dma((6, 4 * PIECES)),
            dma((6,)),
            dma((2,)),
            dma((2,)),
            dma((2,)),
            dma((2,)),
        ],
        compiler_params=pltpu.CompilerParams(collective_id=0, has_side_effects=True, vmem_limit_bytes=44 * 2**20),
        name="mixture",
    )(
        stay(policy_hidden.T),
        stay(ref_hidden.T),
        stay(mix_num.reshape(8, 128)),
        stay(mix_den.reshape(8, 128)),
        stay(policy_unembed),
        stay(ref_unembed),
    )


def solution(mesh):
    finer = Mesh(mesh.devices.reshape(8, 4, 4, 2), VROW_VCOL)
    placed = (P(None, VCOL), P(None, VCOL), P(), P(), P(None, VROW_VCOL), P(None, VROW_VCOL))
    return jax.shard_map(
        body, mesh=finer, in_specs=placed, out_specs=P(None, VROW_VCOL), check_vma=False
    )
```
